32 devices in a mesh: rad: 4 (over x, core), harm: 8 (over z, y).
Axes of the slice: x: 2, y: 2, z: 4, core: 2. Of those that a mesh axis runs over, the one named last changes fastest.
Arguments:
- velocity: bfloat16 [3, 16, 2, 256, 256], P(None, 'rad', None, 'harm'), may hold values from -6 to 6
- magnetic: bfloat16 [3, 16, 2, 256, 256], P(None, 'rad', None, 'harm'), may hold values from -6 to 6
- vorticity: bfloat16 [3, 16, 2, 256, 256], P(None, 'rad', None, 'harm'), may hold values from -6 to 6
- current: bfloat16 [3, 16, 2, 256, 256], P(None, 'rad', None, 'harm'), may hold values from -6 to 6
Outputs:
- advection: bfloat16 [3, 16, 2, 256, 256], P(None, 'rad', None, 'harm')
- induction_gradient: bfloat16 [3, 16, 2, 256, 256], P(None, 'rad', None, 'harm')
- energy_spectra: float32 [2, 16, 256], P(None, 'rad')
The draws below stay inside these ranges and needn't reach their ends.
All inputs are finite; a program needn't handle non-finite values.
Results may differ from the reference program's by a relative error of at most 0.01.
Values may be sent and summed in bfloat16 or wider, within the bound.
A program may use at most 64 MiB of HBM per device.

```python
import jax
import jax.numpy as jnp
from jax import lax

L = 256
NTHETA = 384
NPHI = 768
NR = 16


def block_scale(stream_key, extent, split, low, largest):
    factor_of = 1.0
    for axis_at, parts in split:
        draws = jax.random.uniform(jax.random.fold_in(jax.random.fold_in(stream_key, 6), axis_at), (parts,), jnp.float32, low / len(split), largest / len(split))
        factor_of = factor_of * jnp.repeat(jnp.exp(draws), extent[axis_at] // parts).reshape((-1,) + (1,) * (len(extent) - 1 - axis_at))
    return factor_of


def scatter_about(own_key, dims, scale, most, shards=(), held_as=jnp.bfloat16):
    level = block_scale(own_key, dims, shards, -0.22, 0.18) if shards else 1.0
    values = jax.random.normal(own_key, dims, jnp.float32) * scale * level
    return jnp.minimum(jnp.maximum(values, -most), most).astype(held_as)


def setup_inputs(seed: int = 0) -> dict:
    splits = jax.random.split(jax.random.key(seed), 5)
    return {
        "velocity": scatter_about(splits[0], (3, NR, 2, L, L), 1.0, 6.0, ((1, 4), (3, 8))),
        "magnetic": scatter_about(splits[1], (3, NR, 2, L, L), 1.0, 6.0, ((1, 4), (3, 8))),
        "vorticity": scatter_about(splits[2], (3, NR, 2, L, L), 1.0, 6.0, ((1, 4), (3, 8))),
        "current": scatter_about(splits[3], (3, NR, 2, L, L), 1.0, 6.0, ((1, 4), (3, 8))),
    }


def north_table(order_ints, degree_count, theta_count):
    half_rows = theta_count // 2
    row_index = jnp.arange(half_rows, dtype=jnp.float32)
    angles = jnp.pi * (row_index + 0.5) / theta_count
    cosine = jnp.cos(angles)
    sine_theta = jnp.sin(angles)
    order_float = order_ints.astype(jnp.float32)[:, None]
    steps_k = jnp.arange(1, degree_count, dtype=jnp.int32)
    steps_float = steps_k.astype(jnp.float32)
    log_terms = 0.5 * jnp.log((2.0 * steps_float + 1.0) / (2.0 * steps_float))
    log_taken = jnp.where(steps_k[None, :] <= order_ints[:, None], log_terms[None, :], 0.0)
    log_start = 0.5 * jnp.log(jnp.float32(0.5)) + lax.optimization_barrier(jnp.sum(log_taken, axis=1))
    log_sector = log_start[:, None] + order_float * jnp.log(sine_theta)[None, :]
    sectoral = jnp.exp(jnp.maximum(log_sector, -60.0))
    unscale = jnp.exp(jnp.minimum(log_sector + 60.0, 0.0))
    order_col = order_ints[:, None]
    blocks = 16
    per_block = degree_count // blocks

    def advance(state_pair, block_index):
        latest, before = state_pair
        produced = []
        for inner_step in range(per_block):
            degree = block_index * per_block + inner_step
            degree_float = degree.astype(jnp.float32)
            general = degree > order_col + 1
            degree_square = degree_float * degree_float
            order_square = order_float * order_float
            ratio_upper = jnp.where(general, (4.0 * degree_square - 1.0) / jnp.where(general, degree_square - order_square, 1.0), 1.0)
            lower_degree = degree_float - 1.0
            ratio_lower = jnp.where(general, (lower_degree * lower_degree - order_square) / (4.0 * lower_degree * lower_degree - 1.0), 0.0)
            value_general = jnp.sqrt(ratio_upper) * (cosine[None, :] * latest - jnp.sqrt(ratio_lower) * before)
            first_up = jnp.sqrt(2.0 * order_float + 3.0) * cosine[None, :] * sectoral
            new_value = jnp.where(degree < order_col, 0.0, jnp.where(degree == order_col, sectoral, jnp.where(degree == order_col + 1, first_up, value_general)))
            before = latest
            latest = new_value
            produced.append(new_value)
        return ((latest, before), jnp.stack(produced))
    zero_rows = jnp.zeros((order_ints.shape[0], half_rows), jnp.float32)
    state_pair, legendre_raw = lax.scan(advance, (zero_rows, zero_rows), jnp.arange(blocks, dtype=jnp.int32))
    legendre_raw = legendre_raw.reshape(degree_count, order_ints.shape[0], half_rows)
    return jnp.transpose(legendre_raw, (1, 0, 2)) * unscale[:, None, :]

def full_table(north_rows, order_ints):
    degree_count = north_rows.shape[1]
    degrees = jnp.arange(degree_count, dtype=jnp.int32)
    parity = (degrees[None, :] + order_ints[:, None]) % 2
    sign_factor = (1 - 2 * parity).astype(jnp.float32)[:, :, None]
    return jnp.concatenate([north_rows, sign_factor * jnp.flip(north_rows, 2)], 2)

def quadrature(theta_count):
    half_rows = theta_count // 2
    row_index = jnp.arange(half_rows, dtype=jnp.float32)
    angles = jnp.pi * (row_index + 0.5) / theta_count
    wave_number = jnp.arange(1, half_rows + 1, dtype=jnp.float32)
    series = jnp.cos(2.0 * wave_number[None, :] * angles[:, None]) / (4.0 * wave_number[None, :] * wave_number[None, :] - 1.0)
    north_weights = 2.0 / theta_count * (1.0 - 2.0 * lax.optimization_barrier(jnp.sum(series, axis=1)))
    return jnp.concatenate([north_weights, jnp.flip(north_weights, 0)], 0)

def trig_table(degree_count, phi_count):
    orders = jnp.arange(degree_count, dtype=jnp.int32)[:, None]
    points = jnp.arange(phi_count, dtype=jnp.int32)[None, :]
    phase_angle = 2.0 * jnp.pi * (orders * points % phi_count).astype(jnp.float32) / phi_count
    return jnp.stack([jnp.cos(phase_angle), jnp.sin(phase_angle)]).astype(jnp.bfloat16)

def analysis_factor(order_ints, row_weights, degree_count, phi_count):
    mode_weight = jnp.where(order_ints == 0, 1.0, 2.0).astype(jnp.float32)
    return mode_weight[:, None] * float(degree_count) * row_weights[None, :] / float(phi_count)

def energy_weights(order_ints, degree_count):
    degrees = jnp.arange(degree_count, dtype=jnp.int32)
    order_col = order_ints[:, None]
    live_part = (degrees[None, :] >= order_col).astype(jnp.float32)
    inverse_modes = 1.0 / (2.0 * degrees.astype(jnp.float32) + 1.0)
    cosine_weight = jnp.where(order_col == 0, 0.5, 1.0)
    sine_weight = jnp.where(order_col == 0, 0.0, 1.0)
    return jnp.stack([cosine_weight * live_part * inverse_modes[None, :], sine_weight * live_part * inverse_modes[None, :]]).astype(jnp.float32)

def cross_product(first_vec, second_vec):
    return [first_vec[1] * second_vec[2] - first_vec[2] * second_vec[1], first_vec[2] * second_vec[0] - first_vec[0] * second_vec[2], first_vec[0] * second_vec[1] - first_vec[1] * second_vec[0]]

def nonlinear_terms(components):
    velocity_vec = components[0:3]
    magnetic_vec = components[3:6]
    vorticity_vec = components[6:9]
    current_vec = components[9:12]
    lamb_term = cross_product(velocity_vec, vorticity_vec)
    lorentz_term = cross_product(current_vec, magnetic_vec)
    induced = cross_product(velocity_vec, magnetic_vec)
    return [lamb_term[index_c] + lorentz_term[index_c] for index_c in range(3)] + induced

def rounded(values):
    return lax.optimization_barrier(values.astype(jnp.bfloat16)).astype(jnp.float32)

def reference(velocity, magnetic, vorticity, current):
    all_orders = jnp.arange(L, dtype=jnp.int32)
    north_rows = north_table(all_orders, L, NTHETA)
    legendre = rounded(full_table(north_rows, all_orders))
    trig_rows = lax.optimization_barrier(trig_table(L, NPHI)).astype(jnp.float32)
    factor = analysis_factor(all_orders, quadrature(NTHETA), L, NPHI)
    energy_weight = energy_weights(all_orders, L)
    fields = jnp.concatenate([velocity, magnetic, vorticity, current], 0)
    per_shell = jnp.moveaxis(fields, 1, 0)

    def one_shell(spectrum):
        mode_rows = jnp.einsum('crml,mlt->crmt', spectrum.astype(jnp.float32), legendre) * (1.0 / L)
        mode_rows = rounded(mode_rows)
        grid_values = jnp.einsum('crmt,rmp->ctp', mode_rows, trig_rows)
        products = rounded(jnp.stack(nonlinear_terms([grid_values[index_c] for index_c in range(12)])))
        analysed = jnp.einsum('ctp,rmp->crmt', products, trig_rows) * factor[None, None]
        analysed = rounded(analysed)
        spectra = jnp.einsum('crmt,mlt->crml', analysed, legendre)
        square = spectrum[:6].astype(jnp.float32) ** 2
        kinetic = lax.optimization_barrier(jnp.sum(square[:3] * energy_weight[None], axis=(0, 1, 2)))
        magnetic_energy = lax.optimization_barrier(jnp.sum(square[3:] * energy_weight[None], axis=(0, 1, 2)))
        return (spectra[:3].astype(jnp.bfloat16), spectra[3:].astype(jnp.bfloat16), jnp.stack([kinetic, magnetic_energy]))
    advection, induction, energy = lax.map(one_shell, per_shell)
    induction_wide = induction.astype(jnp.float32)
    padded = jnp.pad(induction_wide, ((1, 1), (0, 0), (0, 0), (0, 0), (0, 0)))
    gradient = ((padded[2:] - padded[:-2]) * 0.5).astype(jnp.bfloat16)
    return (jnp.moveaxis(advection, 0, 1), jnp.moveaxis(gradient, 0, 1), jnp.moveaxis(energy, 0, 1))
```

```python
import functools

import jax
import jax.numpy as jnp
import numpy as np
from jax import lax
from jax.experimental import pallas as pl
from jax.experimental.pallas import tpu as pltpu
from jax.sharding import PartitionSpec as P

MESH = pl.DeviceIdType.MESH
PASSES = 2
BF = jnp.bfloat16
F32 = jnp.float32


def tables(degrees, thetas, points, harm_count):
    half = thetas // 2
    angles = np.pi * (np.arange(half) + 0.5) / thetas
    cosine = np.concatenate([np.cos(angles), -np.cos(angles)[::-1]])
    sine = np.concatenate([np.sin(angles), np.sin(angles)[::-1]])
    orders = np.arange(degrees)
    steps = np.arange(1, degrees)
    terms = 0.5 * np.log((2.0 * steps + 1.0) / (2.0 * steps))
    start = 0.5 * np.log(0.5) + np.concatenate([[0.0], np.cumsum(terms)])
    log_sector = start[:, None] + orders[:, None] * np.log(sine)[None, :]
    sectoral = np.exp(np.maximum(log_sector, -60.0)).astype(np.float32)
    unscale = np.exp(np.minimum(log_sector + 60.0, 0.0)).astype(np.float32)
    wave = np.arange(1, half + 1)
    series = np.cos(2.0 * wave[None, :] * angles[:, None]) / (4.0 * wave[None, :] ** 2 - 1.0)
    north = 2.0 / thetas * (1.0 - 2.0 * series.sum(axis=1))
    weights = np.concatenate([north, north[::-1]])
    weights = (weights * degrees / points).astype(np.float32)
    phase = 2.0 * np.pi * ((orders[:, None] * np.arange(points)[None, :]) % points) / points
    trig = np.stack([np.cos(phase), np.sin(phase)])
    trig = trig.reshape(2, harm_count, degrees // harm_count, points)
    trig = trig.transpose(1, 0, 2, 3).reshape(2 * degrees, points).astype(jnp.bfloat16)
    doubled = np.where(orders == 0, 1.0, 2.0).reshape(harm_count, 1, -1)
    doubled = np.broadcast_to(doubled, (harm_count, 2, degrees // harm_count)).reshape(-1, 1)
    analysis = (trig.astype(np.float32) * doubled).astype(jnp.bfloat16)
    return cosine.astype(np.float32), sectoral, unscale, weights, trig.T.copy(), analysis


def wide(column, width):
    return jnp.concatenate([column] * (width // column.shape[1]), axis=1)


def kernel(
    dims,
    cm_ref, x_ref, sect_ref, unscale_ref, w_ref, trig_ref, back_ref, energy_ref,
    out_ref, energy_out,
    tab, rows, outs, send, recv, grid, prod, send2, recv2, folded, spread, energy_all,
    ssem, rsem, ssem2, rsem2, esend, erecv,
):
    harm, shells, groups, modes, degrees, thetas, points, span = dims
    me = lax.axis_index("harm")
    pair_width = 2 * span
    block = min(16, modes)
    q_pairs = 6 // PASSES
    q_rows = 12 // PASSES * shells * 2

    barrier = pltpu.get_barrier_semaphore()
    for step in range(1, harm):
        peer = lax.rem(me + step, harm)
        pl.semaphore_signal(barrier, inc=1, device_id={"harm": peer}, device_id_type=MESH)

    order = (me * modes + lax.broadcasted_iota(jnp.int32, (modes, 128), 0)).astype(F32)
    order_square = order * order
    energy_all[me] = energy_ref[...]

    def table_block(step, carry):
        latest, before, inverse = carry
        for inner in range(16):
            degree = step * 16 + inner
            lf = jnp.full((modes, 128), degree, jnp.int32).astype(F32)
            dd = jnp.maximum(lf * lf - order_square, 1.0) / (4.0 * lf * lf - 1.0)
            guess = lax.rsqrt(dd)
            guess = guess * (1.5 - 0.5 * dd * guess * guess)
            live = lf > order
            alpha = jnp.where(live, guess, 0.0)
            starts = jnp.where(lf == order, 1.0, 0.0)
            new = wide(alpha, thetas) * (x_ref[...] * latest - wide(inverse, thetas) * before)
            new = new + wide(starts, thetas) * sect_ref[...]
            rows[inner] = new * unscale_ref[...]
            before, latest = latest, new
            inverse = jnp.where(live, dd * guess, 0.0)
        tab[:, pl.ds(pl.multiple_of(step * 16, 16), 16), :] = jnp.swapaxes(rows[...], 0, 1).astype(BF)
        return latest, before, inverse

    zero = jnp.zeros((modes, thetas), F32)
    lax.fori_loop(0, degrees // 16, table_block, (zero, zero, jnp.zeros((modes, 128), F32)))

    pl.semaphore_wait(barrier, harm - 1)

    def energy_copy(step):
        peer = lax.rem(me + step, harm)
        return pltpu.make_async_remote_copy(
            src_ref=energy_all.at[me], dst_ref=energy_all.at[me],
            send_sem=esend.at[step], recv_sem=erecv.at[step],
            device_id={"harm": peer}, device_id_type=MESH,
        )

    def forward(q, step):
        peer = lax.rem(me + step, harm)
        return pltpu.make_async_remote_copy(
            src_ref=send.at[peer, pl.ds(q * q_pairs, q_pairs)],
            dst_ref=recv.at[me, pl.ds(q * q_pairs, q_pairs)],
            send_sem=ssem.at[q, step], recv_sem=rsem.at[q, step],
            device_id={"harm": peer}, device_id_type=MESH,
        )

    def backward(pair, step):
        peer = lax.rem(me + step, harm)
        return pltpu.make_async_remote_copy(
            src_ref=send2.at[peer, pair], dst_ref=recv2.at[me, pair],
            send_sem=ssem2.at[pair, step], recv_sem=rsem2.at[pair, step],
            device_id={"harm": peer}, device_id_type=MESH,
        )

    for q in range(PASSES):
        def mode_block(mb, _, q=q):
            def one(i, _):
                m = mb * block + i
                outs[i] = jnp.dot(cm_ref[q, m], tab[m], preferred_element_type=F32) * (1.0 / degrees)
                return 0

            lax.fori_loop(0, block, one, 0)
            turned = jnp.swapaxes(outs[...], 0, 1)
            for s in range(shells):
                for pair in range(q_pairs):
                    for r in range(2):
                        k = (pair * 2 * shells + s) * 2 + r
                        first, second = turned[k], turned[k + 2 * shells]
                        for g in range(groups):
                            cut = slice(g * span, (g + 1) * span)
                            piece = jnp.concatenate([first[:, cut], second[:, cut]], axis=1).astype(BF)
                            at = pl.multiple_of(r * modes + mb * block, block)
                            send[s * groups + g, q * q_pairs + pair, pl.ds(at, block), :] = piece
            return 0

        lax.fori_loop(0, modes // block, mode_block, 0)
        for step in range(1, harm):
            forward(q, step).start()
        recv[me, pl.ds(q * q_pairs, q_pairs)] = send[me, pl.ds(q * q_pairs, q_pairs)]
    for step in range(1, harm):
        energy_copy(step).start()

    chunk = points // 3
    for q in range(PASSES):
        for step in range(1, harm):
            forward(q, step).wait_recv()
        for pair in range(q * q_pairs, (q + 1) * q_pairs):
            arrived = recv[:, pair].reshape(2 * degrees, pair_width)
            for part in range(3):
                cut = pl.ds(part * chunk, chunk)
                grid[pair, cut, :] = jnp.dot(trig_ref[cut, :], arrived, preferred_element_type=F32)

    piece_rows = 32

    def product_rows(i, _):
        at = pl.ds(pl.multiple_of(i * piece_rows, piece_rows), piece_rows)
        both = [grid[pair, at, :] for pair in range(6)]
        c = []
        for pair in range(6):
            c += [both[pair][:, :span], both[pair][:, span:]]
        u, b, w, j = c[0:3], c[3:6], c[6:9], c[9:12]

        def cross(a, d):
            return [a[1] * d[2] - a[2] * d[1], a[2] * d[0] - a[0] * d[2], a[0] * d[1] - a[1] * d[0]]

        lamb, lorentz, induced = cross(u, w), cross(j, b), cross(u, b)
        six = [lamb[n] + lorentz[n] for n in range(3)] + induced
        for pair in range(3):
            prod[pair, at, :] = jnp.concatenate([six[2 * pair], six[2 * pair + 1]], axis=1).astype(BF)
        return 0

    lax.fori_loop(0, points // piece_rows, product_rows, 0)

    per = 2 * modes
    for pair in range(3):
        analysed = jnp.dot(back_ref[...], prod[pair], preferred_element_type=F32)
        analysed = (analysed * w_ref[...]).astype(BF)
        send2[:, pair] = analysed.reshape(harm, per, pair_width)
        for step in range(1, harm):
            backward(pair, step).start()
        recv2[me, pair] = send2[me, pair]

    for pair in range(3):
        for step in range(1, harm):
            backward(pair, step).wait_recv()

        def fold_block(mb, _, pair=pair):
            for s in range(shells):
                for r in range(2):
                    at = pl.ds(pl.multiple_of(r * modes + mb * block, block), block)
                    got = [recv2[s * groups + g, pair, at, :].astype(F32) for g in range(groups)]
                    for c in range(2):
                        cut = slice(c * span, (c + 1) * span)
                        spread[(c * shells + s) * 2 + r] = jnp.concatenate([v[:, cut] for v in got], axis=1)
            here = pl.ds(pl.multiple_of(mb * block, block), block)
            folded[here, pl.ds(pair * 4 * shells, 4 * shells), :] = jnp.swapaxes(spread[...], 0, 1).astype(BF)
            return 0

        lax.fori_loop(0, modes // block, fold_block, 0)

    def spectrum(m, _):
        out_ref[m] = lax.dot_general(
            folded[m], tab[m], (((1,), (1,)), ((), ())), preferred_element_type=F32
        ).astype(BF)
        return 0

    lax.fori_loop(0, modes, spectrum, 0)

    for step in range(1, harm):
        energy_copy(step).wait_recv()
    energy_out[...] = jnp.sum(energy_all[...], axis=0)
    for step in range(1, harm):
        energy_copy(step).wait_send()
        for q in range(PASSES):
            forward(q, step).wait_send()
        for pair in range(3):
            backward(pair, step).wait_send()


def with_halo(block, axis):
    count = lax.axis_size(axis)
    up = [(i, i + 1) for i in range(count - 1)]
    down = [(b, a) for a, b in up]
    low = lax.ppermute(block[:, -1:], axis, up)
    high = lax.ppermute(block[:, :1], axis, down)
    return jnp.concatenate([low, block, high], axis=1)


def energy_weights(order_ints, degree_count):
    degrees = jnp.arange(degree_count, dtype=jnp.int32)
    order_col = order_ints[:, None]
    live_part = (degrees[None, :] >= order_col).astype(F32)
    inverse_modes = 1.0 / (2.0 * degrees.astype(F32) + 1.0)
    cosine_weight = jnp.where(order_col == 0, 0.5, 1.0)
    sine_weight = jnp.where(order_col == 0, 0.0, 1.0)
    scaled = live_part * inverse_modes[None, :]
    return jnp.stack([cosine_weight * scaled, sine_weight * scaled])


def local(velocity, magnetic, vorticity, current):
    harm = lax.axis_size("harm")
    me = lax.axis_index("harm")
    _, shells, _, modes, degrees = velocity.shape
    thetas, points = 3 * degrees // 2, 3 * degrees
    groups = harm // shells
    span = thetas // groups
    cosine, sectoral, unscale, weights, synthesis, analysis = tables(degrees, thetas, points, harm)

    own = me * modes + jnp.arange(modes, dtype=jnp.int32)
    energy_weight = energy_weights(own, degrees)
    energy = jnp.stack([
        jnp.sum(field.astype(F32) ** 2 * energy_weight[None, None], axis=(0, 2, 3))
        for field in (velocity, magnetic)
    ]).reshape(2 * shells, degrees)

    fields = jnp.concatenate([velocity, magnetic, vorticity, current], axis=0)
    q_rows = 12 // PASSES * shells * 2
    cm = fields.reshape(PASSES, q_rows, modes, degrees).transpose(0, 2, 1, 3)
    x = jnp.broadcast_to(jnp.asarray(cosine)[None, :], (modes, thetas))
    sect = lax.dynamic_slice_in_dim(jnp.asarray(sectoral), me * modes, modes)
    unsc = lax.dynamic_slice_in_dim(jnp.asarray(unscale), me * modes, modes)
    own_weights = lax.dynamic_slice_in_dim(jnp.asarray(weights), lax.rem(me, groups) * span, span)
    w = jnp.concatenate([own_weights, own_weights])[None, :]

    block = min(16, modes)
    vmem = pl.BlockSpec(memory_space=pltpu.VMEM)
    dims = (harm, shells, groups, modes, degrees, thetas, points, span)
    spectra, total = pl.pallas_call(
        functools.partial(kernel, dims),
        name="dynamo",
        out_shape=(
            jax.ShapeDtypeStruct((modes, 12 * shells, degrees), BF),
            jax.ShapeDtypeStruct((2 * shells, degrees), F32),
        ),
        in_specs=[vmem] * 8,
        out_specs=(vmem, vmem),
        scratch_shapes=[
            pltpu.VMEM((modes, degrees, thetas), BF),
            pltpu.VMEM((16, modes, thetas), F32),
            pltpu.VMEM((block, q_rows, thetas), F32),
            pltpu.VMEM((harm, 6, 2 * modes, 2 * span), BF),
            pltpu.VMEM((harm, 6, 2 * modes, 2 * span), BF),
            pltpu.VMEM((6, points, 2 * span), F32),
            pltpu.VMEM((3, points, 2 * span), BF),
            pltpu.VMEM((harm, 3, 2 * modes, 2 * span), BF),
            pltpu.VMEM((harm, 3, 2 * modes, 2 * span), BF),
            pltpu.VMEM((modes, 12 * shells, thetas), BF),
            pltpu.VMEM((4 * shells, block, thetas), F32),
            pltpu.VMEM((harm, 2 * shells, degrees), F32),
            pltpu.SemaphoreType.DMA((PASSES, harm)),
            pltpu.SemaphoreType.DMA((PASSES, harm)),
            pltpu.SemaphoreType.DMA((3, harm)),
            pltpu.SemaphoreType.DMA((3, harm)),
            pltpu.SemaphoreType.DMA((harm,)),
            pltpu.SemaphoreType.DMA((harm,)),
        ],
        compiler_params=pltpu.CompilerParams(
            collective_id=0, has_side_effects=True, vmem_limit_bytes=60 * 1024 * 1024
        ),
    )(cm, x, sect, unsc, w, jnp.asarray(synthesis), jnp.asarray(analysis), energy)

    spectra = spectra.transpose(1, 0, 2).reshape(6, shells, 2, modes, degrees)
    rimmed = with_halo(spectra[3:], "rad").astype(F32)
    gradient = ((rimmed[:, 2:] - rimmed[:, :-2]) * 0.5).astype(BF)
    return spectra[:3], gradient, total.reshape(2, shells, degrees)


def solution(mesh):
    spec = P(None, "rad", None, "harm", None)
    return jax.shard_map(
        local,
        mesh=mesh,
        in_specs=(spec,) * 4,
        out_specs=(spec, spec, P(None, "rad", None)),
        check_vma=False,
    )
```

```python
import functools

import jax
import jax.numpy as jnp
import numpy as np
from jax import lax
from jax.experimental import pallas as pl
from jax.experimental.pallas import tpu as pltpu
from jax.sharding import PartitionSpec as P

MESH = pl.DeviceIdType.MESH
PASSES = 2
BF = jnp.bfloat16
F32 = jnp.float32


def tables(degrees, thetas, points, harm_count):
    half = thetas // 2
    angles = np.pi * (np.arange(half) + 0.5) / thetas
    cosine = np.concatenate([np.cos(angles), -np.cos(angles)[::-1]])
    sine = np.concatenate([np.sin(angles), np.sin(angles)[::-1]])
    orders = np.arange(degrees)
    steps = np.arange(1, degrees)
    terms = 0.5 * np.log((2.0 * steps + 1.0) / (2.0 * steps))
    start = 0.5 * np.log(0.5) + np.concatenate([[0.0], np.cumsum(terms)])
    log_sector = start[:, None] + orders[:, None] * np.log(sine)[None, :]
    sectoral = np.exp(np.maximum(log_sector, -60.0)).astype(np.float32)
    unscale = np.exp(np.minimum(log_sector + 60.0, 0.0)).astype(np.float32)
    wave = np.arange(1, half + 1)
    series = np.cos(2.0 * wave[None, :] * angles[:, None]) / (4.0 * wave[None, :] ** 2 - 1.0)
    north = 2.0 / thetas * (1.0 - 2.0 * series.sum(axis=1))
    weights = np.concatenate([north, north[::-1]])
    weights = (weights * degrees / points).astype(np.float32)
    phase = 2.0 * np.pi * ((orders[:, None] * np.arange(points)[None, :]) % points) / points
    trig = np.stack([np.cos(phase), np.sin(phase)])
    trig = trig.reshape(2, harm_count, degrees // harm_count, points)
    trig = trig.transpose(1, 0, 2, 3).reshape(2 * degrees, points).astype(jnp.bfloat16)
    doubled = np.where(orders == 0, 1.0, 2.0).reshape(harm_count, 1, -1)
    doubled = np.broadcast_to(doubled, (harm_count, 2, degrees // harm_count)).reshape(-1, 1)
    analysis = (trig.astype(np.float32) * doubled).astype(jnp.bfloat16)
    return cosine.astype(np.float32), sectoral, unscale, weights, trig.T.copy(), analysis


def wide(column, width):
    return jnp.concatenate([column] * (width // column.shape[1]), axis=1)


def kernel(
    dims,
    cm_ref, x_ref, sect_ref, unscale_ref, w_ref, trig_ref, back_ref, energy_ref,
    out_ref, energy_out,
    tab, rows, outs, send, recv, grid, prod, send2, recv2, folded, spread, energy_all,
    ssem, rsem, ssem2, rsem2, esend, erecv,
):
    harm, shells, groups, modes, degrees, thetas, points, span = dims
    me = lax.axis_index("harm")
    pair_width = 2 * span
    block = min(16, modes)
    q_pairs = 6 // PASSES
    q_rows = 12 // PASSES * shells * 2

    barrier = pltpu.get_barrier_semaphore()
    for step in range(1, harm):
        peer = lax.rem(me + step, harm)
        pl.semaphore_signal(barrier, inc=1, device_id={"harm": peer}, device_id_type=MESH)

    order = (me * modes + lax.broadcasted_iota(jnp.int32, (modes, 128), 0)).astype(F32)
    order_square = order * order
    own = pl.ds(pl.multiple_of(me * modes, modes), modes)
    energy_all[me] = energy_ref[...]

    def table_block(step, carry):
        latest, before, inverse = carry
        for inner in range(16):
            degree = step * 16 + inner
            lf = jnp.full((modes, 128), degree, jnp.int32).astype(F32)
            dd = jnp.maximum(lf * lf - order_square, 1.0) / (4.0 * lf * lf - 1.0)
            guess = lax.rsqrt(dd)
            guess = guess * (1.5 - 0.5 * dd * guess * guess)
            live = lf > order
            alpha = jnp.where(live, guess, 0.0)
            starts = jnp.where(lf == order, 1.0, 0.0)
            new = wide(alpha, thetas) * (x_ref[...] * latest - wide(inverse, thetas) * before)
            new = new + wide(starts, thetas) * sect_ref[own, :]
            rows[inner] = new * unscale_ref[own, :]
            before, latest = latest, new
            inverse = jnp.where(live, dd * guess, 0.0)
        tab[:, pl.ds(pl.multiple_of(step * 16, 16), 16), :] = jnp.swapaxes(rows[...], 0, 1).astype(BF)
        return latest, before, inverse

    zero = jnp.zeros((modes, thetas), F32)
    lax.fori_loop(0, degrees // 16, table_block, (zero, zero, jnp.zeros((modes, 128), F32)))

    pl.semaphore_wait(barrier, harm - 1)

    def energy_copy(step):
        peer = lax.rem(me + step, harm)
        return pltpu.make_async_remote_copy(
            src_ref=energy_all.at[me], dst_ref=energy_all.at[me],
            send_sem=esend.at[step], recv_sem=erecv.at[step],
            device_id={"harm": peer}, device_id_type=MESH,
        )

    def forward(q, step):
        peer = lax.rem(me + step, harm)
        return pltpu.make_async_remote_copy(
            src_ref=send.at[peer, pl.ds(q * q_pairs, q_pairs)],
            dst_ref=recv.at[me, pl.ds(q * q_pairs, q_pairs)],
            send_sem=ssem.at[q, step], recv_sem=rsem.at[q, step],
            device_id={"harm": peer}, device_id_type=MESH,
        )

    def backward(pair, step):
        peer = lax.rem(me + step, harm)
        return pltpu.make_async_remote_copy(
            src_ref=send2.at[peer, pair], dst_ref=recv2.at[me, pair],
            send_sem=ssem2.at[pair, step], recv_sem=rsem2.at[pair, step],
            device_id={"harm": peer}, device_id_type=MESH,
        )

    for q in range(PASSES):
        def mode_block(mb, _, q=q):
            def one(i, _):
                m = mb * block + i
                outs[i] = jnp.dot(cm_ref[q, m], tab[m], preferred_element_type=F32) * (1.0 / degrees)
                return 0

            lax.fori_loop(0, block, one, 0, unroll=4)
            turned = jnp.swapaxes(outs[...], 0, 1)
            for s in range(shells):
                for pair in range(q_pairs):
                    for r in range(2):
                        k = (pair * 2 * shells + s) * 2 + r
                        first, second = turned[k], turned[k + 2 * shells]
                        for g in range(groups):
                            cut = slice(g * span, (g + 1) * span)
                            piece = jnp.concatenate([first[:, cut], second[:, cut]], axis=1).astype(BF)
                            at = pl.multiple_of(r * modes + mb * block, block)
                            send[s * groups + g, q * q_pairs + pair, pl.ds(at, block), :] = piece
            return 0

        lax.fori_loop(0, modes // block, mode_block, 0)
        for step in range(1, harm):
            forward(q, step).start()
        recv[me, pl.ds(q * q_pairs, q_pairs)] = send[me, pl.ds(q * q_pairs, q_pairs)]
    for step in range(1, harm):
        energy_copy(step).start()

    chunk = points // 3
    for q in range(PASSES):
        for step in range(1, harm):
            forward(q, step).wait_recv()
        for pair in range(q * q_pairs, (q + 1) * q_pairs):
            arrived = recv[:, pair].reshape(2 * degrees, pair_width)
            for part in range(3):
                cut = pl.ds(part * chunk, chunk)
                grid[pair, cut, :] = jnp.dot(trig_ref[cut, :], arrived, preferred_element_type=F32)

    piece_rows = 32

    def product_rows(i, _):
        at = pl.ds(pl.multiple_of(i * piece_rows, piece_rows), piece_rows)
        both = [grid[pair, at, :] for pair in range(6)]
        c = []
        for pair in range(6):
            c += [both[pair][:, :span], both[pair][:, span:]]
        u, b, w, j = c[0:3], c[3:6], c[6:9], c[9:12]

        def cross(a, d):
            return [a[1] * d[2] - a[2] * d[1], a[2] * d[0] - a[0] * d[2], a[0] * d[1] - a[1] * d[0]]

        lamb, lorentz, induced = cross(u, w), cross(j, b), cross(u, b)
        six = [lamb[n] + lorentz[n] for n in range(3)] + induced
        for pair in range(3):
            prod[pair, at, :] = jnp.concatenate([six[2 * pair], six[2 * pair + 1]], axis=1).astype(BF)
        return 0

    lax.fori_loop(0, points // piece_rows, product_rows, 0)

    per = 2 * modes
    for pair in range(3):
        analysed = jnp.dot(back_ref[...], prod[pair], preferred_element_type=F32)
        analysed = (analysed * w_ref[lax.rem(me, groups)]).astype(BF)
        send2[:, pair] = analysed.reshape(harm, per, pair_width)
        for step in range(1, harm):
            backward(pair, step).start()
        recv2[me, pair] = send2[me, pair]

    for pair in range(3):
        for step in range(1, harm):
            backward(pair, step).wait_recv()

        def fold_block(mb, _, pair=pair):
            for s in range(shells):
                for r in range(2):
                    at = pl.ds(pl.multiple_of(r * modes + mb * block, block), block)
                    got = [recv2[s * groups + g, pair, at, :].astype(F32) for g in range(groups)]
                    for c in range(2):
                        cut = slice(c * span, (c + 1) * span)
                        spread[(c * shells + s) * 2 + r] = jnp.concatenate([v[:, cut] for v in got], axis=1)
            here = pl.ds(pl.multiple_of(mb * block, block), block)
            folded[here, pl.ds(pair * 4 * shells, 4 * shells), :] = jnp.swapaxes(spread[...], 0, 1).astype(BF)
            return 0

        lax.fori_loop(0, modes // block, fold_block, 0)

    def spectrum(m, _):
        out_ref[m] = lax.dot_general(
            folded[m], tab[m], (((1,), (1,)), ((), ())), preferred_element_type=F32
        ).astype(BF)
        return 0

    lax.fori_loop(0, modes, spectrum, 0, unroll=4)

    for step in range(1, harm):
        energy_copy(step).wait_recv()
    energy_out[...] = jnp.sum(energy_all[...], axis=0)
    for step in range(1, harm):
        energy_copy(step).wait_send()
        for q in range(PASSES):
            forward(q, step).wait_send()
        for pair in range(3):
            backward(pair, step).wait_send()


def with_halo(block, axis):
    count = lax.axis_size(axis)
    up = [(i, i + 1) for i in range(count - 1)]
    down = [(b, a) for a, b in up]
    low = lax.ppermute(block[:, -1:], axis, up)
    high = lax.ppermute(block[:, :1], axis, down)
    return jnp.concatenate([low, block, high], axis=1)


def energy_weights(order_ints, degree_count):
    degrees = jnp.arange(degree_count, dtype=jnp.int32)
    order_col = order_ints[:, None]
    live_part = (degrees[None, :] >= order_col).astype(F32)
    inverse_modes = 1.0 / (2.0 * degrees.astype(F32) + 1.0)
    cosine_weight = jnp.where(order_col == 0, 0.5, 1.0)
    sine_weight = jnp.where(order_col == 0, 0.0, 1.0)
    scaled = live_part * inverse_modes[None, :]
    return jnp.stack([cosine_weight * scaled, sine_weight * scaled])


def local(velocity, magnetic, vorticity, current):
    harm = lax.axis_size("harm")
    me = lax.axis_index("harm")
    _, shells, _, modes, degrees = velocity.shape
    thetas, points = 3 * degrees // 2, 3 * degrees
    groups = harm // shells
    span = thetas // groups
    cosine, sectoral, unscale, weights, synthesis, analysis = tables(degrees, thetas, points, harm)

    own = me * modes + jnp.arange(modes, dtype=jnp.int32)
    energy_weight = energy_weights(own, degrees)
    energy = jnp.stack([
        jnp.sum(field.astype(F32) ** 2 * energy_weight[None, None], axis=(0, 2, 3))
        for field in (velocity, magnetic)
    ])

    fields = jnp.concatenate([velocity, magnetic, vorticity, current], axis=0)
    q_rows = 12 // PASSES * shells * 2
    cm = fields.reshape(PASSES, q_rows, modes, degrees).transpose(0, 2, 1, 3)
    x = jnp.asarray(np.broadcast_to(cosine[None, :], (modes, thetas)).copy())
    cut_weights = weights.reshape(groups, 1, span)
    w = jnp.asarray(np.concatenate([cut_weights, cut_weights], axis=2))

    block = min(16, modes)
    vmem = pl.BlockSpec(memory_space=pltpu.VMEM)
    dims = (harm, shells, groups, modes, degrees, thetas, points, span)
    spectra, total = pl.pallas_call(
        functools.partial(kernel, dims),
        name="dynamo",
        out_shape=(
            jax.ShapeDtypeStruct((modes, 12 * shells, degrees), BF),
            jax.ShapeDtypeStruct((2, shells, degrees), F32),
        ),
        in_specs=[vmem] * 8,
        out_specs=(vmem, vmem),
        scratch_shapes=[
            pltpu.VMEM((modes, degrees, thetas), BF),
            pltpu.VMEM((16, modes, thetas), F32),
            pltpu.VMEM((block, q_rows, thetas), F32),
            pltpu.VMEM((harm, 6, 2 * modes, 2 * span), BF),
            pltpu.VMEM((harm, 6, 2 * modes, 2 * span), BF),
            pltpu.VMEM((6, points, 2 * span), F32),
            pltpu.VMEM((3, points, 2 * span), BF),
            pltpu.VMEM((harm, 3, 2 * modes, 2 * span), BF),
            pltpu.VMEM((harm, 3, 2 * modes, 2 * span), BF),
            pltpu.VMEM((modes, 12 * shells, thetas), BF),
            pltpu.VMEM((4 * shells, block, thetas), F32),
            pltpu.VMEM((harm, 2, shells, degrees), F32),
            pltpu.SemaphoreType.DMA((PASSES, harm)),
            pltpu.SemaphoreType.DMA((PASSES, harm)),
            pltpu.SemaphoreType.DMA((3, harm)),
            pltpu.SemaphoreType.DMA((3, harm)),
            pltpu.SemaphoreType.DMA((harm,)),
            pltpu.SemaphoreType.DMA((harm,)),
        ],
        compiler_params=pltpu.CompilerParams(
            collective_id=0, has_side_effects=True, vmem_limit_bytes=60 * 1024 * 1024
        ),
    )(cm, x, jnp.asarray(sectoral), jnp.asarray(unscale), w, jnp.asarray(synthesis), jnp.asarray(analysis), energy)

    spectra = spectra.transpose(1, 0, 2).reshape(6, shells, 2, modes, degrees)
    rimmed = with_halo(spectra[3:], "rad").astype(F32)
    gradient = ((rimmed[:, 2:] - rimmed[:, :-2]) * 0.5).astype(BF)
    return spectra[:3], gradient, total


def solution(mesh):
    spec = P(None, "rad", None, "harm", None)
    return jax.shard_map(
        local,
        mesh=mesh,
        in_specs=(spec,) * 4,
        out_specs=(spec, spec, P(None, "rad", None)),
        check_vma=False,
    )
```
